256 devices in a mesh: graph: 64 (over z, y, core), feat: 4 (over x).
Axes of the slice: x: 4, y: 4, z: 8, core: 2. Of those that a mesh axis runs over, the one named last changes fastest.
Arguments:
- node_feats: bfloat16 [20480, 512], P(('graph', 'feat')), may hold values from -6 to 6
- edge_feats: bfloat16 [131072, 512], P(('graph', 'feat')), may hold values from -6 to 6
- senders: int32 [131072], P(('graph', 'feat')), may hold values from 0 to 319
- receiver_ref: int32 [131072], P(('graph', 'feat')), may hold values from 0 to 6463, as said below
- send_list: int32 [64, 64, 96], P('graph'), may hold values from 0 to 319, as said below
- edge_count: int32 [64], P('graph'), may hold values from 1024 to 2048, as said below
- edge_w1: bfloat16 [1536, 512], replicated, may hold values from -0.15625 to 0.15625
- edge_w2: bfloat16 [512, 512], replicated, may hold values from -0.25 to 0.25
- edge_gain: bfloat16 [512], replicated, may hold values from 0.099609375 to 1.8984375
- edge_shift: bfloat16 [512], replicated, may hold values from -3 to 3
- node_w1: bfloat16 [1024, 512], replicated, may hold values from -0.1875 to 0.1875
- node_w2: bfloat16 [512, 512], replicated, may hold values from -0.25 to 0.25
- node_gain: bfloat16 [512], replicated, may hold values from 0.099609375 to 1.8984375
- node_shift: bfloat16 [512], replicated, may hold values from -3 to 3
Outputs:
- new_edges: bfloat16 [131072, 512], P(('graph', 'feat'))
- new_nodes: bfloat16 [20480, 512], P(('graph', 'feat'))
The draws below stay inside these ranges and needn't reach their ends.
Inputs may be any that keep to these rules, and one draw needn't show every extreme that they name: `senders`: local node indices of the edge's own region. `receiver_ref`: A value below 320 is a node of the edge's own region. Otherwise q = value - 320 names slot q % 96 of the list that region s = q // 96 keeps for the edge's region; s is never the edge's own region, and when s is more than 2 steps away around the region order (either direction, wrapping) the slot is below 16. In every draw each region has an edge on slot 95 of the next region and an edge on slot 15 of the region 3 steps on. Each list send_list[s, g] holds 96 distinct local node indices of region s. Region g's live edges are its first edge_count[g] edge slots; some region has all 2048 live.
All inputs are finite; a program needn't handle non-finite values.
Results may differ from the reference program's by a relative error of at most 0.009.
Values may be sent and summed in bfloat16 or wider, within the bound.
A program may use at most 128 MiB of HBM per device.

```python
import jax
import jax.numpy as jnp
from jax import lax

D = 512
HID = 512
NODE_DEV = 320
EDGE_DEV = 2048
SLOT = 96
FAR_SLOT = 16
REACH = 2
NODES = 20480
EDGES = 131072
N_GRAPH = 64


def draw_send_list(key, part):
    random_scores = jax.random.randint(key, (N_GRAPH * N_GRAPH, NODE_DEV), 0, 1 << 16)
    distinct_scores = random_scores * NODE_DEV + jnp.arange(NODE_DEV, dtype=jnp.int32)[None, :]
    ranked = jnp.argsort(distinct_scores, axis=1, stable=True)[:, :SLOT]
    return ranked.reshape(N_GRAPH, N_GRAPH, SLOT).astype(jnp.int32)


def draw_receiver_ref(key, part):
    subkeys = jax.random.split(key, 5)
    total_edges = N_GRAPH * EDGE_DEV
    shard_index = jnp.arange(total_edges, dtype=jnp.int32) // EDGE_DEV
    position = jnp.arange(total_edges, dtype=jnp.int32) % EDGE_DEV
    category = jax.random.randint(subkeys[0], (total_edges,), 0, 10)
    local_node = jax.random.randint(subkeys[1], (total_edges,), 0, NODE_DEV)
    near_pick = jax.random.randint(subkeys[2], (total_edges,), 0, 2 * REACH)
    near_offset = jnp.where(near_pick < REACH, near_pick - REACH, near_pick - REACH + 1)
    far_offset = REACH + 1 + jax.random.randint(subkeys[3], (total_edges,), 0, N_GRAPH - 2 * REACH - 1)
    near_slot = jax.random.randint(subkeys[4], (total_edges,), 0, SLOT)
    far_slot = near_slot % FAR_SLOT
    near_offset = jnp.where(position == 1, 1, near_offset)
    near_slot = jnp.where(position == 1, SLOT - 1, near_slot)
    far_offset = jnp.where(position == 0, REACH + 1, far_offset)
    far_slot = jnp.where(position == 0, FAR_SLOT - 1, far_slot)
    category = jnp.where(position == 0, 0, jnp.where(position == 1, 1, category))
    near_value = NODE_DEV + (shard_index + near_offset) % N_GRAPH * SLOT + near_slot
    far_value = NODE_DEV + (shard_index + far_offset) % N_GRAPH * SLOT + far_slot
    return jnp.where(category == 0, far_value, jnp.where(category < 5, near_value, local_node)).astype(jnp.int32)


def draw_edge_count(key, part):
    count_key, full_key = jax.random.split(key)
    edge_totals = jax.random.randint(count_key, (N_GRAPH,), EDGE_DEV // 2, EDGE_DEV + 1)
    fullest = jax.random.randint(full_key, (), 0, N_GRAPH)
    return jnp.where(jnp.arange(N_GRAPH) == fullest, EDGE_DEV, edge_totals).astype(jnp.int32)


def place_ends(drawn, rng, low, largest):
    index_at = [jax.random.randint(jax.random.fold_in(rng, axis), (), 0, length) for axis, length in enumerate(drawn.shape)]
    main_axis = drawn.shape.index(max(drawn.shape))
    neighbour = index_at[:main_axis] + [(index_at[main_axis] + 1) % drawn.shape[main_axis]] + index_at[main_axis + 1:]
    return drawn.at[tuple(index_at)].set(low).at[tuple(neighbour)].set(largest)


def levels(stream_key, dims, cuts, low, high):
    loudness, own = 1.0, jax.random.fold_in(stream_key, 6)
    for dim, parts in cuts:
        steps = jnp.exp(jax.random.uniform(jax.random.fold_in(own, dim), (parts,), jnp.float32, low / len(cuts), high / len(cuts)))
        loudness = loudness * jnp.repeat(steps, dims[dim] // parts).reshape([-1 if axis == dim else 1 for axis in range(len(dims))])
    return loudness


def centred(stream_key, dims, width, reach, pieces=(), kind=jnp.bfloat16):
    entries = width * jax.random.normal(stream_key, dims, jnp.float32)
    if pieces:
        entries = entries * levels(stream_key, dims, pieces, -0.22, 0.18)
    return jnp.clip(entries, -reach, reach).astype(kind)


def setup_inputs(seed: int = 0) -> dict:
    splits = jax.random.split(jax.random.key(seed), 15)
    node_feats = centred(splits[0], (NODES, D), 1.0, 6.0, ((0, 256),))
    edge_feats = centred(splits[1], (EDGES, D), 1.0, 6.0, ((0, 256),))
    senders = place_ends(jax.random.randint(splits[2], (EDGES,), 0, NODE_DEV), jax.random.fold_in(splits[2], 1), 0, NODE_DEV - 1).astype(jnp.int32)
    receiver_ref = draw_receiver_ref(jax.random.fold_in(splits[14], 71), 0)
    send_list = draw_send_list(jax.random.fold_in(splits[14], 71), 0)
    edge_count = draw_edge_count(jax.random.fold_in(splits[14], 71), 0)
    edge_w1 = centred(splits[6], (3 * D, HID), (3 * D) ** -0.5, 0.15625)
    edge_w2 = centred(splits[7], (HID, D), HID ** -0.5, 0.25)
    edge_gain = jnp.clip(1.0 + 0.18 * jax.random.normal(splits[8], (D,), jnp.float32), 0.099609375, 1.8984375).astype(jnp.bfloat16)
    edge_shift = centred(splits[9], (D,), 0.5, 3.0)
    node_w1 = centred(splits[10], (2 * D, HID), (2 * D) ** -0.5, 0.1875)
    node_w2 = centred(splits[11], (HID, D), HID ** -0.5, 0.25)
    node_gain = jnp.clip(1.0 + 0.18 * jax.random.normal(splits[12], (D,), jnp.float32), 0.099609375, 1.8984375).astype(jnp.bfloat16)
    node_shift = centred(splits[13], (D,), 0.5, 3.0)
    return dict(node_feats=node_feats, edge_feats=edge_feats, senders=senders, receiver_ref=receiver_ref, send_list=send_list, edge_count=edge_count, edge_w1=edge_w1, edge_w2=edge_w2, edge_gain=edge_gain, edge_shift=edge_shift, node_w1=node_w1, node_w2=node_w2, node_gain=node_gain, node_shift=node_shift)


epsilon = 1e-05

def layer_norm(outputs, norm_gain, norm_shift):
    average = lax.optimization_barrier(jnp.mean(outputs, axis=-1, keepdims=True))
    centered = outputs - average
    variance = lax.optimization_barrier(jnp.mean(centered * centered, axis=-1, keepdims=True))
    return centered * lax.rsqrt(variance + epsilon) * norm_gain + norm_shift

def perceptron(inputs, first_weight, second_weight, norm_gain, norm_shift):
    joined = jnp.concatenate(inputs, axis=1)
    activation = jnp.dot(joined, first_weight, preferred_element_type=jnp.float32)
    hidden = jax.nn.silu(activation).astype(jnp.bfloat16)
    outputs = jnp.dot(hidden, second_weight, preferred_element_type=jnp.float32)
    return layer_norm(outputs, norm_gain, norm_shift)

def reference(node_feats, edge_feats, senders, receiver_ref, send_list, edge_count, edge_w1, edge_w2, edge_gain, edge_shift, node_w1, node_w2, node_gain, node_shift):
    positions = jnp.arange(EDGE_DEV, dtype=jnp.int32)

    def shard_step(aggregate, shard_index):
        first_edge = shard_index * EDGE_DEV
        edge_block = lax.dynamic_slice_in_dim(edge_feats, first_edge, EDGE_DEV, 0)
        sender_block = lax.dynamic_slice_in_dim(senders, first_edge, EDGE_DEV, 0)
        ref_block = lax.dynamic_slice_in_dim(receiver_ref, first_edge, EDGE_DEV, 0)
        offset = jnp.maximum(ref_block - NODE_DEV, 0)
        source = offset // SLOT
        slot_index = offset % SLOT
        column = lax.dynamic_index_in_dim(send_list, shard_index, 1, keepdims=False)
        remote = source * NODE_DEV + column[source, slot_index]
        receivers = jnp.where(ref_block < NODE_DEV, shard_index * NODE_DEV + ref_block, remote).astype(jnp.int32)
        sender_rows = node_feats[(shard_index * NODE_DEV + sender_block).astype(jnp.int32)]
        receiver_rows = node_feats[receivers]
        update = edge_block.astype(jnp.float32) + perceptron((edge_block, sender_rows, receiver_rows), edge_w1, edge_w2, edge_gain, edge_shift)
        live_mask = positions < edge_count[shard_index]
        new_rows = jnp.where(live_mask[:, None], update, edge_block.astype(jnp.float32)).astype(jnp.bfloat16)
        messages = jnp.where(live_mask[:, None], new_rows.astype(jnp.float32), 0.0)
        aggregate = aggregate.at[receivers].add(messages)
        return (aggregate, new_rows)
    aggregate, new_edges = lax.scan(shard_step, jnp.zeros((NODES, D), jnp.float32), jnp.arange(N_GRAPH, dtype=jnp.int32))
    new_edges = new_edges.reshape(EDGES, D)
    node_update = node_feats.astype(jnp.float32) + perceptron((node_feats, aggregate.astype(jnp.bfloat16)), node_w1, node_w2, node_gain, node_shift)
    return (new_edges, node_update.astype(jnp.bfloat16))
```

```python
import jax
import jax.numpy as jnp
from jax import lax
from jax.sharding import PartitionSpec as P

NODE_DEV = 320
SLOT = 96
FAR_SLOT = 16
REACH = 2
OFFSETS = (-2, -1, 1, 2)


epsilon = 1e-05


def layer_norm(outputs, norm_gain, norm_shift):
    average = jnp.mean(outputs, axis=-1, keepdims=True)
    centered = outputs - average
    variance = jnp.mean(centered * centered, axis=-1, keepdims=True)
    return centered * lax.rsqrt(variance + epsilon) * norm_gain + norm_shift


def perceptron(inputs, first_weight, second_weight, norm_gain, norm_shift):
    joined = jnp.concatenate(inputs, axis=1)
    activation = jnp.dot(joined, first_weight, preferred_element_type=jnp.float32)
    hidden = jax.nn.silu(activation).astype(jnp.bfloat16)
    outputs = jnp.dot(hidden, second_weight, preferred_element_type=jnp.float32)
    return layer_norm(outputs, norm_gain, norm_shift)


def one_hot_rows(indices, width):
    return (indices[:, None] == lax.iota(jnp.int32, width)[None, :]).astype(jnp.bfloat16)


def pick(selector, values):
    return jnp.dot(selector, values, preferred_element_type=jnp.float32).astype(jnp.bfloat16)


def sum_into(selector, values):
    return lax.dot_general(
        selector, values, (((0,), (0,)), ((), ())), preferred_element_type=jnp.float32
    )


def exchange(tiles, axis):
    return lax.all_to_all(tiles, axis, split_axis=0, concat_axis=0, tiled=True)


def passed_along(value, axis, by):
    devices = lax.axis_size(axis)
    return lax.ppermute(value, axis, [(i, (i + by) % devices) for i in range(devices)])


def everywhere(value, axis):
    devices = lax.axis_size(axis)
    return exchange(jnp.broadcast_to(value[None], (devices, *value.shape)), axis)


def quarters(value, parts):
    rows, width = value.shape
    return jnp.moveaxis(value.reshape(rows, parts, width // parts), 1, 0)


def rejoined(tiles):
    parts, rows, width = tiles.shape
    return jnp.moveaxis(tiles, 0, 1).reshape(rows, parts * width)


def per_device(
    node_feats,
    edge_feats,
    senders,
    receiver_ref,
    send_list,
    edge_count,
    edge_w1,
    edge_w2,
    edge_gain,
    edge_shift,
    node_w1,
    node_w2,
    node_gain,
    node_shift,
):
    width = node_feats.shape[1]
    edge_local = edge_feats.shape[0]
    groups = lax.axis_size("graph")
    parts = lax.axis_size("feat")
    own = lax.axis_index("graph")
    share = lax.axis_index("feat")
    quarter = width // parts
    far_rows = groups * FAR_SLOT
    table_rows = far_rows + len(OFFSETS) * SLOT

    region_nodes = everywhere(node_feats, "feat").reshape(NODE_DEV, width)
    all_refs = everywhere(receiver_ref[None], "feat").reshape(-1)
    my_nodes = lax.dynamic_slice_in_dim(region_nodes, share * quarter, quarter, 1)

    send_rows = send_list[0]
    near_lists = [
        lax.dynamic_index_in_dim(send_rows, (own + d) % groups, 0, keepdims=False) for d in OFFSETS
    ]
    out_rows = jnp.concatenate([send_rows[:, :FAR_SLOT].reshape(-1), *near_lists])
    list_select = one_hot_rows(out_rows, NODE_DEV)
    outgoing = pick(list_select, my_nodes)
    far_part = exchange(outgoing[:far_rows].reshape(groups, FAR_SLOT, quarter), "graph")
    near_part = []
    for n, d in enumerate(OFFSETS):
        block = outgoing[far_rows + n * SLOT : far_rows + (n + 1) * SLOT]
        near_part.append(passed_along(block, "graph", d))
    table = jnp.concatenate([far_part.reshape(far_rows, quarter), *near_part])

    offset = jnp.maximum(all_refs - NODE_DEV, 0)
    source = offset // SLOT
    slot = offset % SLOT
    row = source * FAR_SLOT + slot
    for n, d in enumerate(OFFSETS):
        row = jnp.where(source == (own - d) % groups, far_rows + n * SLOT + slot, row)
    row = jnp.where(all_refs < NODE_DEV, -1, row)
    own_row = jnp.where(all_refs < NODE_DEV, all_refs, -1)
    table_select = one_hot_rows(row, table_rows)

    picked = pick(table_select, table).reshape(parts, edge_local, quarter)
    away_rows = rejoined(exchange(picked, "feat"))
    sender_rows = pick(one_hot_rows(senders, NODE_DEV), region_nodes)
    local_rows = pick(one_hot_rows(receiver_ref, NODE_DEV), region_nodes)
    receiver_rows = local_rows + away_rows

    update = edge_feats.astype(jnp.float32) + perceptron(
        (edge_feats, sender_rows, receiver_rows), edge_w1, edge_w2, edge_gain, edge_shift
    )
    live = share * edge_local + lax.iota(jnp.int32, edge_local) < edge_count[0]
    new_edges = jnp.where(live[:, None], update, edge_feats.astype(jnp.float32)).astype(
        jnp.bfloat16
    )
    messages = jnp.where(live[:, None], new_edges, jnp.zeros_like(new_edges))
    arrived = exchange(quarters(messages, parts), "feat").reshape(parts * edge_local, quarter)
    away_sums = sum_into(table_select, arrived).astype(jnp.bfloat16)
    own_sums = sum_into(one_hot_rows(own_row, NODE_DEV), arrived)
    far_back = exchange(away_sums[:far_rows].reshape(groups, FAR_SLOT, quarter), "graph")
    near_back = []
    for n, d in enumerate(OFFSETS):
        block = away_sums[far_rows + n * SLOT : far_rows + (n + 1) * SLOT]
        near_back.append(passed_along(block, "graph", -d))
    returned = jnp.concatenate([far_back.reshape(far_rows, quarter), *near_back])
    totals = (own_sums + sum_into(list_select, returned)).astype(jnp.bfloat16)
    aggregate = rejoined(exchange(totals.reshape(parts, NODE_DEV // parts, quarter), "feat"))
    node_update = node_feats.astype(jnp.float32) + perceptron(
        (node_feats, aggregate), node_w1, node_w2, node_gain, node_shift
    )
    return (new_edges, node_update.astype(jnp.bfloat16))


def solution(mesh):
    return jax.shard_map(
        per_device,
        mesh=mesh,
        in_specs=(
            P(("graph", "feat"), None),
            P(("graph", "feat"), None),
            P(("graph", "feat")),
            P(("graph", "feat")),
            P("graph", None, None),
            P("graph"),
            P(),
            P(),
            P(),
            P(),
            P(),
            P(),
            P(),
            P(),
        ),
        out_specs=(P(("graph", "feat"), None), P(("graph", "feat"), None)),
        check_vma=False,
    )
```

```python
import functools

import jax
import jax.numpy as jnp
from jax import lax
from jax.experimental import pallas as pl
from jax.experimental.pallas import tpu as pltpu
from jax.sharding import PartitionSpec as P

NODE_DEV = 320
NODE_PAD = 384
SLOT = 96
FAR_SLOT = 16
REACH = 2
OFFSETS = (-2, -1, 1, 2)
LANES = 128
CHUNKS = 4

epsilon = 1e-05

BF16 = jnp.bfloat16
F32 = jnp.float32


def dot(a, b):
    return jnp.dot(a, b, preferred_element_type=F32)


def one_hot(cond):
    return jnp.where(cond, 1.0, 0.0).astype(BF16)


def silu(v):
    return v / (1.0 + jnp.exp(-v))


def layer_norm(outputs, gain, shift):
    average = jnp.mean(outputs, axis=-1, keepdims=True)
    centered = outputs - average
    variance = jnp.mean(centered * centered, axis=-1, keepdims=True)
    return centered * lax.rsqrt(variance + epsilon) * gain + shift


def await_bytes(ref, sem):
    pltpu.make_async_copy(ref, ref, sem).wait()


def step_kernel(
    groups,
    parts,
    node_ref,
    edge_hbm,
    snd_ref,
    ref_ref,
    list_ref,
    cnt_ref,
    w1_hbm,
    w2_hbm,
    eg_ref,
    es_ref,
    nw1_hbm,
    nw2_hbm,
    ng_ref,
    ns_ref,
    out_edges_hbm,
    out_nodes_ref,
    w1,
    w2,
    nw1,
    nw2,
    edges,
    region,
    refs,
    lists,
    lsel,
    lsel_t,
    table,
    outgoing,
    sel,
    sel_t,
    rows_row,
    base,
    picked,
    pieces,
    updated,
    sent,
    msgs,
    acc,
    back_out,
    returned,
    totals,
    agg,
    load_sem,
    f1_send,
    f1_recv,
    fr_send,
    fr_recv,
    far_send,
    far_recv,
    near_send,
    near_recv,
    f3_send,
    f3_recv,
    b1_send,
    b1_recv,
    bfar_send,
    bfar_recv,
    bnear_send,
    bnear_recv,
    b3_send,
    b3_recv,
    store_sem,
):
    own = lax.axis_index("graph")
    share = lax.axis_index("feat")
    far_rows = groups * FAR_SLOT
    table_rows = far_rows + len(OFFSETS) * SLOT
    edge_local = edge_hbm.shape[0]
    width = edge_hbm.shape[1]
    quarter = width // parts
    node_local = node_ref.shape[0]
    ce = edge_local // CHUNKS
    cw = parts * ce

    def graph_peer(i):
        return lax.rem(own + i, groups)

    def feat_peer(j):
        return lax.rem(share + j, parts)

    def near_target(d):
        return lax.rem(own + d + groups, groups)

    barrier = pltpu.get_barrier_semaphore()
    for j in range(1, parts):
        pl.semaphore_signal(barrier, inc=1, device_id={"feat": feat_peer(j)})

    @pl.loop(1, groups)
    def _(i):
        pl.semaphore_signal(barrier, inc=1, device_id={"graph": graph_peer(i)})

    loads = [
        pltpu.make_async_copy(src, dst, load_sem.at[n])
        for n, (src, dst) in enumerate(
            ((edge_hbm, edges), (w1_hbm, w1), (w2_hbm, w2), (nw1_hbm, nw1), (nw2_hbm, nw2))
        )
    ]
    for load in loads:
        load.start()

    lists[...] = jnp.zeros_like(lists)
    lists[: groups, :SLOT] = list_ref[...]
    turned = lists[...].T
    lane = lax.broadcasted_iota(jnp.int32, (FAR_SLOT, NODE_PAD), 1)
    for s in range(groups):
        ids = jnp.broadcast_to(turned[:FAR_SLOT, s : s + 1], (FAR_SLOT, NODE_PAD))
        lsel[s * FAR_SLOT : (s + 1) * FAR_SLOT, :] = one_hot(ids == lane)
    lane = lax.broadcasted_iota(jnp.int32, (SLOT, LANES), 1)
    for n, d in enumerate(OFFSETS):
        ids = lists[pl.ds(near_target(d), 1), :]
        ids = jnp.broadcast_to(ids, (LANES, LANES)).T[:SLOT, :]
        first = far_rows + n * SLOT
        for t in range(NODE_PAD // LANES):
            lsel[first : first + SLOT, t * LANES : (t + 1) * LANES] = one_hot(ids == lane + t * LANES)

    own_block = pl.ds(pl.multiple_of(own * FAR_SLOT, FAR_SLOT), FAR_SLOT)
    table[own_block, :] = jnp.zeros((FAR_SLOT, quarter), BF16)
    returned[own_block, :] = jnp.zeros((FAR_SLOT, quarter), BF16)
    region[NODE_DEV:, :] = jnp.zeros((NODE_PAD - NODE_DEV, width), BF16)
    own_nodes = pl.ds(pl.multiple_of(share * node_local, 16), node_local)
    region[own_nodes, :] = node_ref[...]
    refs[pl.ds(share, 1)] = ref_ref[...][None]

    pl.semaphore_wait(barrier, groups - 1 + parts - 1)

    sends = []
    for j in range(1, parts):
        to = {"feat": feat_peer(j)}
        sends.append(
            pltpu.make_async_remote_copy(
                src_ref=node_ref,
                dst_ref=region.at[own_nodes],
                send_sem=f1_send.at[j],
                recv_sem=f1_recv.at[share],
                device_id=to,
            )
        )
        sends.append(
            pltpu.make_async_remote_copy(
                src_ref=ref_ref,
                dst_ref=refs.at[share],
                send_sem=fr_send.at[j],
                recv_sem=fr_recv.at[share],
                device_id=to,
            )
        )
    for send in sends:
        send.start()
    for j in range(1, parts):
        p = feat_peer(j)
        await_bytes(
            region.at[pl.ds(pl.multiple_of(p * node_local, 16), node_local)], f1_recv.at[p]
        )

    my_lanes = pl.ds(pl.multiple_of(share * quarter, LANES), quarter)
    outgoing[...] = dot(lsel[...], region[:, my_lanes]).astype(BF16)

    def far_copy(i, source, target, send_sem, recv_sem):
        peer = graph_peer(i)
        return pltpu.make_async_remote_copy(
            src_ref=source.at[pl.ds(pl.multiple_of(peer * FAR_SLOT, FAR_SLOT), FAR_SLOT)],
            dst_ref=target.at[own_block],
            send_sem=send_sem,
            recv_sem=recv_sem,
            device_id={"graph": peer},
        )

    def near_copy(n, d, source, target, send_sem, recv_sem):
        block = pl.ds(far_rows + n * SLOT, SLOT)
        return pltpu.make_async_remote_copy(
            src_ref=source.at[block],
            dst_ref=target.at[block],
            send_sem=send_sem.at[n],
            recv_sem=recv_sem.at[n],
            device_id={"graph": near_target(d)},
        )

    near_out = [
        near_copy(n, d, outgoing, table, near_send, near_recv) for n, d in enumerate(OFFSETS)
    ]
    for send in near_out:
        send.start()

    @pl.loop(1, groups)
    def _(i):
        far_copy(i, outgoing, table, far_send, far_recv).start()

    for j in range(1, parts):
        p = feat_peer(j)
        await_bytes(refs.at[p], fr_recv.at[p])
    for p in range(parts):
        value = refs[p]
        offset = jnp.maximum(value - NODE_DEV, 0)
        source = lax.shift_right_logical(offset * 10923, 20)
        slot = offset - source * SLOT
        row = source * FAR_SLOT + slot
        for n, d in enumerate(OFFSETS):
            row = jnp.where(source == near_target(-d), far_rows + n * SLOT + slot, row)
        row = jnp.where(value < NODE_DEV, table_rows + value, row)
        for c in range(CHUNKS):
            first = c * cw + p * ce
            rows_row[:, first : first + ce] = row[:, c * ce : (c + 1) * ce]

    @pl.loop(0, CHUNKS * cw // LANES)
    def _(b):
        at = pl.multiple_of(b * LANES, LANES)
        ids = jnp.broadcast_to(rows_row[:, pl.ds(at, LANES)], (LANES, LANES)).T
        lanes = lax.broadcasted_iota(jnp.int32, (LANES, LANES), 1)
        for t in range(table_rows // LANES):
            sel[pl.ds(at, LANES), t * LANES : (t + 1) * LANES] = one_hot(ids == lanes + t * LANES)

    for load in loads[:2]:
        load.wait()

    block = 64

    @pl.loop(0, (table_rows + NODE_DEV) // block)
    def _(b):
        at = pl.multiple_of(b * block, block)
        for k in range(0, CHUNKS * cw, 512):
            subs = lax.broadcasted_iota(jnp.int32, (block, 512), 0) + at
            ids = jnp.broadcast_to(rows_row[:, k : k + 512], (block, 512))
            sel_t[pl.ds(at, block), k : k + 512] = one_hot(ids == subs)

    @pl.loop(0, edge_local // LANES)
    def _(b):
        at = pl.multiple_of(b * LANES, LANES)
        lanes = lax.broadcasted_iota(jnp.int32, (LANES, LANES), 1)
        rows = []
        for ids_ref in (snd_ref, ref_ref):
            ids = jnp.broadcast_to(ids_ref[:, pl.ds(at, LANES)], (LANES, LANES)).T
            chosen = jnp.concatenate(
                [one_hot(ids == lanes + t * LANES) for t in range(NODE_PAD // LANES)], axis=1
            )
            rows.append(dot(chosen, region[...]).astype(BF16))
        joined = jnp.concatenate([edges[pl.ds(at, LANES), :], *rows], axis=1)
        base[pl.ds(at, LANES), :] = dot(joined, w1[...])

    for t in range(NODE_PAD // LANES):
        for r in range(table_rows // LANES):
            tile = lsel[r * LANES : (r + 1) * LANES, t * LANES : (t + 1) * LANES]
            lsel_t[t * LANES : (t + 1) * LANES, r * LANES : (r + 1) * LANES] = (
                tile.astype(F32).T.astype(BF16)
            )

    for load in loads[2:]:
        load.wait()
    node_base = dot(node_ref[...], nw1[:width, :])

    for n in range(len(OFFSETS)):
        await_bytes(table.at[pl.ds(far_rows + n * SLOT, SLOT)], near_recv.at[n])
    await_bytes(table.at[pl.ds(0, far_rows - FAR_SLOT)], far_recv)

    def rows_for(c, p):
        at = pl.multiple_of(c * cw + p * ce, ce)
        return dot(sel[pl.ds(at, ce), :], table[...]).astype(BF16)

    row_sends = []
    for c in range(CHUNKS):
        for j in (2, 1, 3):
            p = feat_peer(j)
            picked[c, j] = rows_for(c, p)
            send = pltpu.make_async_remote_copy(
                src_ref=picked.at[c, j],
                dst_ref=pieces.at[c, share],
                send_sem=f3_send.at[c, j],
                recv_sem=f3_recv.at[c, share],
                device_id={"feat": p},
            )
            send.start()
            row_sends.append(send)
        pieces[c, pl.ds(share, 1)] = rows_for(c, share)[None]

    gain = eg_ref[...].astype(F32)
    shift = es_ref[...].astype(F32)
    count = cnt_ref[0]
    message_sends = []
    for c in range(CHUNKS):
        for j in range(1, parts):
            p = feat_peer(j)
            await_bytes(pieces.at[c, p], f3_recv.at[c, p])
        at = c * ce
        away = jnp.concatenate([pieces[c, p] for p in range(parts)], axis=1)
        pre = base[at : at + ce, :] + dot(away, w1[2 * width :, :])
        outputs = dot(silu(pre).astype(BF16), w2[...])
        before = edges[at : at + ce, :]
        update = before.astype(F32) + layer_norm(outputs, gain, shift)
        index = lax.broadcasted_iota(jnp.int32, (ce, width), 0) + (share * edge_local + at)
        live = index < count
        fresh = jnp.where(live, update, before.astype(F32))
        updated[at : at + ce, :] = fresh.astype(BF16)
        message = jnp.where(live, fresh, 0.0).astype(BF16)
        for p in range(parts):
            sent[c, p] = message[:, p * quarter : (p + 1) * quarter]
        for j in (2, 1, 3):
            p = feat_peer(j)
            send = pltpu.make_async_remote_copy(
                src_ref=sent.at[c, p],
                dst_ref=msgs.at[c, share],
                send_sem=b1_send.at[c, j],
                recv_sem=b1_recv.at[c, share],
                device_id={"feat": p},
            )
            send.start()
            message_sends.append(send)
        msgs[c, pl.ds(share, 1)] = sent[c, pl.ds(share, 1)]
    store = pltpu.make_async_copy(updated, out_edges_hbm, store_sem)
    store.start()

    for c in range(CHUNKS):
        for j in range(1, parts):
            p = feat_peer(j)
            await_bytes(msgs.at[c, p], b1_recv.at[c, p])
        part = dot(
            sel_t[:, c * cw : (c + 1) * cw], msgs[c].reshape(cw, quarter)
        )
        if c == 0:
            acc[...] = part
        elif c < CHUNKS - 1:
            acc[...] += part
        else:
            part = acc[...] + part
            back_out[...] = part[:table_rows].astype(BF16)
            acc[table_rows:, :] = part[table_rows:]

    def near_return(n, d):
        block = pl.ds(far_rows + n * SLOT, SLOT)
        return pltpu.make_async_remote_copy(
            src_ref=back_out.at[block],
            dst_ref=returned.at[block],
            send_sem=bnear_send.at[n],
            recv_sem=bnear_recv.at[n],
            device_id={"graph": near_target(-d)},
        )

    near_back = [near_return(n, d) for n, d in enumerate(OFFSETS)]
    for send in near_back:
        send.start()

    @pl.loop(1, groups)
    def _(i):
        far_copy(i, back_out, returned, bfar_send, bfar_recv).start()

    for n in range(len(OFFSETS)):
        await_bytes(returned.at[pl.ds(far_rows + n * SLOT, SLOT)], bnear_recv.at[n])
    await_bytes(returned.at[pl.ds(0, far_rows - FAR_SLOT)], bfar_recv)

    totals[...] = (
        acc[table_rows:, :] + dot(lsel_t[...], returned[...])[:NODE_DEV]
    ).astype(BF16)
    total_sends = []
    for j in range(1, parts):
        p = feat_peer(j)
        send = pltpu.make_async_remote_copy(
            src_ref=totals.at[pl.ds(pl.multiple_of(p * node_local, 16), node_local)],
            dst_ref=agg.at[share],
            send_sem=b3_send.at[j],
            recv_sem=b3_recv.at[share],
            device_id={"feat": p},
        )
        send.start()
        total_sends.append(send)
    agg[pl.ds(share, 1)] = totals[own_nodes, :][None]
    for j in range(1, parts):
        p = feat_peer(j)
        await_bytes(agg.at[p], b3_recv.at[p])

    aggregate = jnp.concatenate([agg[p] for p in range(parts)], axis=1)
    pre = node_base + dot(aggregate, nw1[width:, :])
    outputs = dot(silu(pre).astype(BF16), nw2[...])
    out_nodes_ref[...] = (
        node_ref[...].astype(F32)
        + layer_norm(outputs, ng_ref[...].astype(F32), ns_ref[...].astype(F32))
    ).astype(BF16)

    for send in sends + near_out + row_sends + message_sends + near_back + total_sends:
        send.wait_send()
    await_bytes(outgoing.at[pl.ds(0, far_rows - FAR_SLOT)], far_send)
    await_bytes(back_out.at[pl.ds(0, far_rows - FAR_SLOT)], bfar_send)
    store.wait()


def per_device(
    node_feats,
    edge_feats,
    senders,
    receiver_ref,
    send_list,
    edge_count,
    edge_w1,
    edge_w2,
    edge_gain,
    edge_shift,
    node_w1,
    node_w2,
    node_gain,
    node_shift,
):
    groups = lax.axis_size("graph")
    parts = lax.axis_size("feat")
    node_local, width = node_feats.shape
    edge_local = edge_feats.shape[0]
    quarter = width // parts
    far_rows = groups * FAR_SLOT
    table_rows = far_rows + len(OFFSETS) * SLOT
    edge_region = parts * edge_local
    ce = edge_local // CHUNKS
    near = len(OFFSETS)
    vmem = pl.BlockSpec(memory_space=pltpu.VMEM)
    smem = pl.BlockSpec(memory_space=pltpu.SMEM)
    hbm = pl.BlockSpec(memory_space=pl.ANY)
    dma = pltpu.SemaphoreType.DMA
    return pl.pallas_call(
        functools.partial(step_kernel, groups, parts),
        out_shape=(
            jax.ShapeDtypeStruct(edge_feats.shape, BF16),
            jax.ShapeDtypeStruct(node_feats.shape, BF16),
        ),
        in_specs=[
            vmem, hbm, vmem, vmem, vmem, smem, hbm, hbm, vmem, vmem, hbm, hbm, vmem, vmem,
        ],
        out_specs=(hbm, vmem),
        scratch_shapes=[
            pltpu.VMEM(edge_w1.shape, BF16),
            pltpu.VMEM(edge_w2.shape, BF16),
            pltpu.VMEM(node_w1.shape, BF16),
            pltpu.VMEM(node_w2.shape, BF16),
            pltpu.VMEM(edge_feats.shape, BF16),
            pltpu.VMEM((NODE_PAD, width), BF16),
            pltpu.VMEM((parts, 1, edge_local), jnp.int32),
            pltpu.VMEM((LANES, LANES), jnp.int32),
            pltpu.VMEM((table_rows, NODE_PAD), BF16),
            pltpu.VMEM((NODE_PAD, table_rows), BF16),
            pltpu.VMEM((table_rows, quarter), BF16),
            pltpu.VMEM((table_rows, quarter), BF16),
            pltpu.VMEM((edge_region, table_rows), BF16),
            pltpu.VMEM((table_rows + NODE_DEV, edge_region), BF16),
            pltpu.VMEM((1, edge_region), jnp.int32),
            pltpu.VMEM((edge_local, width), F32),
            pltpu.VMEM((CHUNKS, parts, ce, quarter), BF16),
            pltpu.VMEM((CHUNKS, parts, ce, quarter), BF16),
            pltpu.VMEM(edge_feats.shape, BF16),
            pltpu.VMEM((CHUNKS, parts, ce, quarter), BF16),
            pltpu.VMEM((CHUNKS, parts, ce, quarter), BF16),
            pltpu.VMEM((table_rows + NODE_DEV, quarter), F32),
            pltpu.VMEM((table_rows, quarter), BF16),
            pltpu.VMEM((table_rows, quarter), BF16),
            pltpu.VMEM((NODE_DEV, quarter), BF16),
            pltpu.VMEM((parts, node_local, quarter), BF16),
            dma((5,)),
            dma((parts,)),
            dma((parts,)),
            dma((parts,)),
            dma((parts,)),
            dma,
            dma,
            dma((near,)),
            dma((near,)),
            dma((CHUNKS, parts)),
            dma((CHUNKS, parts)),
            dma((CHUNKS, parts)),
            dma((CHUNKS, parts)),
            dma,
            dma,
            dma((near,)),
            dma((near,)),
            dma((parts,)),
            dma((parts,)),
            dma,
        ],
        compiler_params=pltpu.CompilerParams(
            collective_id=0, has_side_effects=True, vmem_limit_bytes=56 * 2**20
        ),
        name="step",
    )(
        node_feats,
        edge_feats,
        senders.reshape(1, -1),
        receiver_ref.reshape(1, -1),
        send_list[0],
        edge_count,
        edge_w1,
        edge_w2,
        edge_gain.reshape(1, -1),
        edge_shift.reshape(1, -1),
        node_w1,
        node_w2,
        node_gain.reshape(1, -1),
        node_shift.reshape(1, -1),
    )


def solution(mesh):
    return jax.shard_map(
        per_device,
        mesh=mesh,
        in_specs=(
            P(("graph", "feat"), None),
            P(("graph", "feat"), None),
            P(("graph", "feat")),
            P(("graph", "feat")),
            P("graph", None, None),
            P("graph"),
            P(),
            P(),
            P(),
            P(),
            P(),
            P(),
            P(),
            P(),
        ),
        out_specs=(P(("graph", "feat"), None), P(("graph", "feat"), None)),
        check_vma=False,
    )
```

```python
import functools

import jax
import jax.numpy as jnp
from jax import lax
from jax.experimental import pallas as pl
from jax.experimental.pallas import tpu as pltpu
from jax.sharding import PartitionSpec as P

NODE_DEV = 320
NODE_PAD = 384
SLOT = 96
FAR_SLOT = 16
REACH = 2
OFFSETS = (-2, -1, 1, 2)
LANES = 128
ROW = 4
PAIR = 2
CHUNKS = 4

epsilon = 1e-05

BF16 = jnp.bfloat16
F32 = jnp.float32


def dot(a, b):
    return jnp.dot(a, b, preferred_element_type=F32)


def one_hot(cond):
    return jnp.where(cond, 1.0, 0.0).astype(BF16)


def silu(v):
    return v / (1.0 + jnp.exp(-v))


def layer_norm(outputs, gain, shift):
    average = jnp.mean(outputs, axis=-1, keepdims=True)
    centered = outputs - average
    variance = jnp.mean(centered * centered, axis=-1, keepdims=True)
    return centered * lax.rsqrt(variance + epsilon) * gain + shift


class Phases:
    def __init__(self):
        self.scope = None

    def __call__(self, name):
        self.end()
        self.scope = jax.named_scope(name)
        self.scope.__enter__()

    def end(self):
        if self.scope is not None:
            self.scope.__exit__(None, None, None)
            self.scope = None


def in_hbm(value):
    return pltpu.with_memory_space_constraint(value, pltpu.HBM)


def await_bytes(ref, sem):
    pltpu.make_async_copy(ref, ref, sem).wait()


def step_kernel(
    groups,
    parts,
    node_hbm,
    edge_hbm,
    snd_hbm,
    ref_hbm,
    list_hbm,
    cnt_ref,
    w1_hbm,
    w2_hbm,
    eg_hbm,
    es_hbm,
    nw1_hbm,
    nw2_hbm,
    ng_hbm,
    ns_hbm,
    new_edges,
    new_nodes,
    nodes,
    edges,
    snd_ref,
    ref_ref,
    list_ref,
    w1,
    w2,
    eg_ref,
    es_ref,
    nw1,
    nw2,
    ng_ref,
    ns_ref,
    region,
    refs,
    lists,
    lsel,
    lsel_t,
    table,
    outgoing,
    sel,
    sel_t,
    rows_row,
    base,
    picked,
    pieces,
    sent,
    msgs,
    acc,
    back_out,
    returned,
    totals,
    agg,
    node_sem,
    load_sem,
    row_in,
    pair_in,
    f1_send,
    f1_recv,
    fr_send,
    fr_recv,
    f2_send,
    f2_recv,
    f3_send,
    f3_recv,
    b1_send,
    b1_recv,
    b2_send,
    b2_recv,
    b3_send,
    b3_recv,
):
    own = lax.axis_index("graph")
    share = lax.axis_index("feat")
    far_rows = groups * FAR_SLOT
    table_rows = far_rows + len(OFFSETS) * SLOT
    edge_local = edge_hbm.shape[0]
    width = edge_hbm.shape[1]
    quarter = width // parts
    node_local = node_hbm.shape[0]
    ce = edge_local // CHUNKS
    cw = parts * ce

    def graph_peer(i):
        return lax.rem(own + i, groups)

    def feat_peer(j):
        return lax.rem(share + j, parts)

    def near_target(d):
        return lax.rem(own + d + groups, groups)

    place = lax.rem(own, ROW * PAIR)
    core = lax.rem(own, PAIR)
    pair_peer = own + 1 - 2 * core

    def row_peer(i):
        return own - place + lax.rem(place + i * PAIR, ROW * PAIR)

    phase = Phases()
    phase("signal")
    barrier = pltpu.get_barrier_semaphore()
    line = groups // (ROW * PAIR)
    for i in sorted(range(1, line), key=lambda z: -min(z, line - z)):
        at = lax.rem(own + i * ROW * PAIR, groups)
        pl.semaphore_signal(barrier, inc=1, device_id={"graph": at})
    for j in range(1, parts):
        pl.semaphore_signal(barrier, inc=1, device_id={"feat": feat_peer(j)})
    for i in range(1, ROW):
        pl.semaphore_signal(barrier, inc=1, device_id={"graph": row_peer(i)})
    pl.semaphore_signal(barrier, inc=1, device_id={"graph": pair_peer})
    for p in range(parts):
        pltpu.make_async_copy(
            node_hbm.at[:, p * quarter : (p + 1) * quarter], nodes.at[p], node_sem
        ).start()
    loads = [
        pltpu.make_async_copy(src, dst, load_sem.at[n])
        for n, (src, dst) in enumerate(
            (
                (ref_hbm, ref_ref),
                (list_hbm, list_ref),
                (snd_hbm, snd_ref),
                (edge_hbm, edges),
                (w1_hbm, w1),
                (w2_hbm, w2),
                (eg_hbm, eg_ref),
                (es_hbm, es_ref),
                (nw1_hbm, nw1),
                (nw2_hbm, nw2),
                (ng_hbm, ng_ref),
                (ns_hbm, ns_ref),
            )
        )
    ]
    for load in loads[:2]:
        load.start()

    phase("prep")
    own_block = pl.ds(pl.multiple_of(own * FAR_SLOT, FAR_SLOT), FAR_SLOT)
    table[own_block, :] = jnp.zeros((FAR_SLOT, quarter), BF16)
    returned[own_block, :] = jnp.zeros((FAR_SLOT, quarter), BF16)
    region[:, NODE_DEV:, :] = jnp.zeros((parts, NODE_PAD - NODE_DEV, quarter), BF16)
    own_nodes = pl.ds(pl.multiple_of(share * node_local, 16), node_local)
    loads[0].wait()
    await_bytes(nodes, node_sem)
    region[:, own_nodes, :] = nodes[...]
    refs[pl.ds(share, 1)] = ref_ref[...][None]

    phase("barrier")
    pl.semaphore_wait(barrier, line - 1 + parts - 1 + ROW - 1 + 1)

    sends = []
    for j in (2, 1, 3):
        p = feat_peer(j)
        sends.append(
            pltpu.make_async_remote_copy(
                src_ref=nodes.at[p],
                dst_ref=region.at[p, own_nodes],
                send_sem=f1_send,
                recv_sem=f1_recv.at[0],
                device_id={"feat": p},
            )
        )
    for j in (2, 1, 3):
        p = feat_peer(j)
        sends.append(
            pltpu.make_async_remote_copy(
                src_ref=ref_ref,
                dst_ref=refs.at[share],
                send_sem=fr_send,
                recv_sem=fr_recv,
                device_id={"feat": p},
            )
        )
    for send in sends:
        send.start()

    for load in loads[2:]:
        load.start()

    for i in range(1, ROW):
        pl.semaphore_signal(row_in, inc=1, device_id={"graph": row_peer(i)})

    phase("lists")
    lists[...] = jnp.zeros_like(lists)
    loads[1].wait()
    lists[: groups, :SLOT] = list_ref[...]
    turned = lists[...].T
    lane = lax.broadcasted_iota(jnp.int32, (FAR_SLOT, NODE_PAD), 1)
    for s in range(groups):
        ids = jnp.broadcast_to(turned[:FAR_SLOT, s : s + 1], (FAR_SLOT, NODE_PAD))
        lsel[s * FAR_SLOT : (s + 1) * FAR_SLOT, :] = one_hot(ids == lane)
    lane = lax.broadcasted_iota(jnp.int32, (SLOT, LANES), 1)
    for n, d in enumerate(OFFSETS):
        ids = lists[pl.ds(near_target(d), 1), :]
        ids = jnp.broadcast_to(ids, (LANES, LANES)).T[:SLOT, :]
        first = far_rows + n * SLOT
        for t in range(NODE_PAD // LANES):
            lsel[first : first + SLOT, t * LANES : (t + 1) * LANES] = one_hot(ids == lane + t * LANES)

    phase("rows_in")
    pl.semaphore_wait(row_in, ROW - 1)
    pl.semaphore_signal(pair_in, inc=1, device_id={"graph": pair_peer})
    pl.semaphore_wait(pair_in, 1)

    phase("f1_wait")

    others = pl.ds(0, (parts - 1) * node_local)
    await_bytes(region.at[0, others], f1_recv.at[0])

    phase("list_dot")
    outgoing[...] = dot(lsel[...], region[share]).astype(BF16)

    def exchange(source, target, sign, send_sem, recv_sem):
        def far(i):
            peer = graph_peer(i)
            return pltpu.make_async_remote_copy(
                src_ref=source.at[pl.ds(pl.multiple_of(peer * FAR_SLOT, FAR_SLOT), FAR_SLOT)],
                dst_ref=target.at[own_block],
                send_sem=send_sem,
                recv_sem=recv_sem,
                device_id={"graph": peer},
            )

        def send_far():
            plane = ROW * PAIR
            for dz in sorted(range(line), key=lambda z: -min(z, line - z)):
                first = dz * plane + (dz == 0)

                @pl.loop(first, (dz + 1) * plane, unroll=True)
                def _(i):
                    far(i).start()

        def send_near():
            for n, d in enumerate(OFFSETS):
                block = pl.ds(far_rows + n * SLOT, SLOT)
                pltpu.make_async_remote_copy(
                    src_ref=source.at[block],
                    dst_ref=target.at[block],
                    send_sem=send_sem,
                    recv_sem=recv_sem,
                    device_id={"graph": near_target(sign * d)},
                ).start()

        return send_far, send_near

    passed = pl.ds(0, table_rows - FAR_SLOT)
    phase("f2_start")
    for send in exchange(outgoing, table, 1, f2_send, f2_recv):
        send()

    for i in range(1, parts):
        for j in (2, 1, 3):
            p = feat_peer(j)
            q = lax.rem(p + i, parts)
            pltpu.make_async_remote_copy(
                src_ref=nodes.at[q],
                dst_ref=region.at[q, own_nodes],
                send_sem=f1_send,
                recv_sem=f1_recv.at[1],
                device_id={"feat": p},
            ).start()

    await_bytes(refs.at[pl.ds(0, parts - 1)], fr_recv)
    for p in range(parts):
        value = refs[p]
        offset = jnp.maximum(value - NODE_DEV, 0)
        source = lax.shift_right_logical(offset * 10923, 20)
        slot = offset - source * SLOT
        row = source * FAR_SLOT + slot
        for n, d in enumerate(OFFSETS):
            row = jnp.where(source == near_target(-d), far_rows + n * SLOT + slot, row)
        row = jnp.where(value < NODE_DEV, table_rows + value, row)
        for c in range(CHUNKS):
            first = c * cw + p * ce
            rows_row[:, first : first + ce] = row[:, c * ce : (c + 1) * ce]

    phase("sel")
    @pl.loop(0, CHUNKS * cw // LANES)
    def _(b):
        at = pl.multiple_of(b * LANES, LANES)
        ids = jnp.broadcast_to(rows_row[:, pl.ds(at, LANES)], (LANES, LANES)).T
        lanes = lax.broadcasted_iota(jnp.int32, (LANES, LANES), 1)
        for t in range(table_rows // LANES):
            sel[pl.ds(at, LANES), t * LANES : (t + 1) * LANES] = one_hot(ids == lanes + t * LANES)

    phase("load_wait")
    for load in loads[2:5]:
        load.wait()

    phase("sel_t")
    block = 64

    @pl.loop(0, (table_rows + NODE_DEV) // block)
    def _(b):
        at = pl.multiple_of(b * block, block)
        for k in range(0, CHUNKS * cw, 512):
            subs = lax.broadcasted_iota(jnp.int32, (block, 512), 0) + at
            ids = jnp.broadcast_to(rows_row[:, k : k + 512], (block, 512))
            sel_t[pl.ds(at, block), k : k + 512] = one_hot(ids == subs)

    phase("f1b_wait")
    await_bytes(region.at[pl.ds(0, parts - 1), others], f1_recv.at[1])
    phase("base")
    @pl.loop(0, edge_local // LANES)
    def _(b):
        at = pl.multiple_of(b * LANES, LANES)
        lanes = lax.broadcasted_iota(jnp.int32, (LANES, LANES), 1)
        rows = []
        for ids_ref in (snd_ref, ref_ref):
            ids = jnp.broadcast_to(ids_ref[:, pl.ds(at, LANES)], (LANES, LANES)).T
            chosen = jnp.concatenate(
                [one_hot(ids == lanes + t * LANES) for t in range(NODE_PAD // LANES)], axis=1
            )
            whole = jnp.concatenate([region[p] for p in range(parts)], axis=1)
            rows.append(dot(chosen, whole).astype(BF16))
        joined = jnp.concatenate([edges[pl.ds(at, LANES), :], *rows], axis=1)
        base[pl.ds(at, LANES), :] = dot(joined, w1[...])

    for load in loads[5:8]:
        load.wait()

    phase("f2_wait")
    await_bytes(table.at[passed], f2_recv)
    phase("pick")
    def send_rows(c, p):
        pltpu.make_async_remote_copy(
            src_ref=picked.at[c, p],
            dst_ref=pieces.at[c, share],
            send_sem=f3_send,
            recv_sem=f3_recv.at[c],
            device_id={"feat": p},
        ).start()

    for j in (2, 1, 3, 0):
        p = feat_peer(j)
        at = pl.ds(pl.multiple_of(p * ce, ce), ce)
        picked[0, pl.ds(p, 1)] = dot(sel[at, :], table[...]).astype(BF16)[None]
        if j:
            send_rows(0, p)
    for c in range(1, CHUNKS):
        picked[c] = (
            dot(sel[c * cw : (c + 1) * cw, :], table[...]).astype(BF16).reshape(parts, ce, quarter)
        )
        for j in (2, 1, 3):
            send_rows(c, feat_peer(j))
    pieces[:, pl.ds(share, 1)] = picked[:, pl.ds(share, 1)]

    gain = eg_ref[...].astype(F32)[None]
    shift = es_ref[...].astype(F32)[None]
    count = cnt_ref[0]
    for c in range(CHUNKS):
        phase("f3_wait")
        await_bytes(pieces.at[c, pl.ds(0, parts - 1)], f3_recv.at[c])
        phase("mlp")
        at = c * ce
        away = jnp.concatenate([pieces[c, p] for p in range(parts)], axis=1)
        pre = base[at : at + ce, :] + dot(away, w1[2 * width :, :])
        outputs = dot(silu(pre).astype(BF16), w2[...])
        before = edges[at : at + ce, :]
        update = before.astype(F32) + layer_norm(outputs, gain, shift)
        index = lax.broadcasted_iota(jnp.int32, (ce, width), 0) + (share * edge_local + at)
        live = index < count
        new_edges[at : at + ce, :] = jnp.where(live, update, before.astype(F32)).astype(BF16)
        message = jnp.where(live, update, 0.0).astype(BF16)
        for p in range(parts):
            sent[c, p] = message[:, p * quarter : (p + 1) * quarter]
        for j in (2, 1, 3):
            p = feat_peer(j)
            pltpu.make_async_remote_copy(
                src_ref=sent.at[c, p],
                dst_ref=msgs.at[c, share],
                send_sem=b1_send,
                recv_sem=b1_recv.at[c],
                device_id={"feat": p},
            ).start()
        msgs[c, pl.ds(share, 1)] = sent[c, pl.ds(share, 1)]

    for c in range(CHUNKS):
        phase("b1_wait")
        await_bytes(msgs.at[c, pl.ds(0, parts - 1)], b1_recv.at[c])
        phase("seg_sum")
        columns = slice(c * cw, (c + 1) * cw)
        message = msgs[c].reshape(cw, quarter)
        if c == 0:
            acc[...] = dot(sel_t[:, columns], message)
        elif c < CHUNKS - 1:
            acc[...] += dot(sel_t[:, columns], message)

    send_far, send_near = exchange(back_out, returned, -1, b2_send, b2_recv)
    back_out[:far_rows] = (acc[:far_rows] + dot(sel_t[:far_rows, columns], message)).astype(BF16)
    phase("b2_start")
    send_far()
    rest = acc[far_rows:] + dot(sel_t[far_rows:, columns], message)
    back_out[far_rows:] = rest[: table_rows - far_rows].astype(BF16)
    acc[table_rows:, :] = rest[table_rows - far_rows :]
    send_near()
    phase("lsel_t")
    for t in range(NODE_PAD // LANES):
        for r in range(table_rows // LANES):
            tile = lsel[r * LANES : (r + 1) * LANES, t * LANES : (t + 1) * LANES]
            lsel_t[t * LANES : (t + 1) * LANES, r * LANES : (r + 1) * LANES] = (
                tile.astype(F32).T.astype(BF16)
            )

    phase("node_base")
    for load in loads[8:]:
        load.wait()
    own_feats = jnp.concatenate([nodes[p] for p in range(parts)], axis=1)
    node_base = dot(own_feats, nw1[:width, :])

    phase("b2_wait")
    await_bytes(returned.at[passed], b2_recv)

    phase("totals")
    totals[...] = (
        acc[table_rows:, :] + dot(lsel_t[...], returned[...])[:NODE_DEV]
    ).astype(BF16)
    for j in range(1, parts):
        p = feat_peer(j)
        pltpu.make_async_remote_copy(
            src_ref=totals.at[pl.ds(pl.multiple_of(p * node_local, 16), node_local)],
            dst_ref=agg.at[share],
            send_sem=b3_send,
            recv_sem=b3_recv,
            device_id={"feat": p},
        ).start()
    agg[pl.ds(share, 1)] = totals[own_nodes, :][None]
    phase("b3_wait")
    await_bytes(agg.at[pl.ds(0, parts - 1)], b3_recv)

    phase("node")
    aggregate = jnp.concatenate([agg[p] for p in range(parts)], axis=1)
    pre = node_base + dot(aggregate, nw1[width:, :])
    outputs = dot(silu(pre).astype(BF16), nw2[...])
    update = own_feats.astype(F32) + layer_norm(
        outputs, ng_ref[...].astype(F32)[None], ns_ref[...].astype(F32)[None]
    )
    new_nodes[...] = update.astype(BF16)

    phase("drain")
    await_bytes(refs.at[pl.ds(0, parts - 1)], fr_send)
    await_bytes(region.at[:, others], f1_send)
    await_bytes(outgoing.at[passed], f2_send)
    await_bytes(picked.at[:, pl.ds(0, parts - 1)], f3_send)
    await_bytes(sent.at[:, pl.ds(0, parts - 1)], b1_send)
    await_bytes(back_out.at[passed], b2_send)
    await_bytes(agg.at[pl.ds(0, parts - 1)], b3_send)
    phase.end()


def hand_out(edges, nodes, edges_out, nodes_out, edge_sem, node_sem):
    copies = (
        pltpu.make_async_copy(edges, edges_out, edge_sem),
        pltpu.make_async_copy(nodes, nodes_out, node_sem),
    )
    for copy in copies:
        copy.start()
    for copy in copies:
        copy.wait()


def per_device(
    node_feats,
    edge_feats,
    senders,
    receiver_ref,
    send_list,
    edge_count,
    edge_w1,
    edge_w2,
    edge_gain,
    edge_shift,
    node_w1,
    node_w2,
    node_gain,
    node_shift,
):
    groups = lax.axis_size("graph")
    parts = lax.axis_size("feat")
    node_local, width = node_feats.shape
    edge_local = edge_feats.shape[0]
    quarter = width // parts
    far_rows = groups * FAR_SLOT
    table_rows = far_rows + len(OFFSETS) * SLOT
    edge_region = parts * edge_local
    ce = edge_local // CHUNKS
    vmem = pl.BlockSpec(memory_space=pltpu.VMEM)
    smem = pl.BlockSpec(memory_space=pltpu.SMEM)
    hbm = pl.BlockSpec(memory_space=pltpu.HBM)
    dma = pltpu.SemaphoreType.DMA
    finished = pl.pallas_call(
        functools.partial(step_kernel, groups, parts),
        out_shape=(
            pltpu.VMEM(edge_feats.shape, BF16),
            pltpu.VMEM(node_feats.shape, BF16),
        ),
        in_specs=[
            hbm, hbm, hbm, hbm, hbm, smem, hbm, hbm, hbm, hbm, hbm, hbm, hbm, hbm,
        ],
        out_specs=(vmem, vmem),
        scratch_shapes=[
            pltpu.VMEM((parts, node_local, quarter), BF16),
            pltpu.VMEM(edge_feats.shape, BF16),
            pltpu.VMEM((1, edge_local), jnp.int32),
            pltpu.VMEM((1, edge_local), jnp.int32),
            pltpu.VMEM((groups, SLOT), jnp.int32),
            pltpu.VMEM(edge_w1.shape, BF16),
            pltpu.VMEM(edge_w2.shape, BF16),
            pltpu.VMEM((width,), BF16),
            pltpu.VMEM((width,), BF16),
            pltpu.VMEM(node_w1.shape, BF16),
            pltpu.VMEM(node_w2.shape, BF16),
            pltpu.VMEM((width,), BF16),
            pltpu.VMEM((width,), BF16),
            pltpu.VMEM((parts, NODE_PAD, quarter), BF16),
            pltpu.VMEM((parts, 1, edge_local), jnp.int32),
            pltpu.VMEM((LANES, LANES), jnp.int32),
            pltpu.VMEM((table_rows, NODE_PAD), BF16),
            pltpu.VMEM((NODE_PAD, table_rows), BF16),
            pltpu.VMEM((table_rows, quarter), BF16),
            pltpu.VMEM((table_rows, quarter), BF16),
            pltpu.VMEM((edge_region, table_rows), BF16),
            pltpu.VMEM((table_rows + NODE_DEV, edge_region), BF16),
            pltpu.VMEM((1, edge_region), jnp.int32),
            pltpu.VMEM((edge_local, width), F32),
            pltpu.VMEM((CHUNKS, parts, ce, quarter), BF16),
            pltpu.VMEM((CHUNKS, parts, ce, quarter), BF16),
            pltpu.VMEM((CHUNKS, parts, ce, quarter), BF16),
            pltpu.VMEM((CHUNKS, parts, ce, quarter), BF16),
            pltpu.VMEM((table_rows + NODE_DEV, quarter), F32),
            pltpu.VMEM((table_rows, quarter), BF16),
            pltpu.VMEM((table_rows, quarter), BF16),
            pltpu.VMEM((NODE_DEV, quarter), BF16),
            pltpu.VMEM((parts, node_local, quarter), BF16),
            dma,
            dma((12,)),
            pltpu.SemaphoreType.REGULAR,
            pltpu.SemaphoreType.REGULAR,
            dma,
            dma((2,)),
            dma,
            dma,
            dma,
            dma,
            dma,
            dma((CHUNKS,)),
            dma,
            dma((CHUNKS,)),
            dma,
            dma,
            dma,
            dma,
        ],
        compiler_params=pltpu.CompilerParams(
            collective_id=0, has_side_effects=True, vmem_limit_bytes=48 * 2**20
        ),
        name="step",
    )(
        in_hbm(node_feats),
        in_hbm(edge_feats),
        in_hbm(senders.reshape(1, -1)),
        in_hbm(receiver_ref.reshape(1, -1)),
        in_hbm(send_list[0]),
        edge_count,
        in_hbm(edge_w1),
        in_hbm(edge_w2),
        in_hbm(edge_gain),
        in_hbm(edge_shift),
        in_hbm(node_w1),
        in_hbm(node_w2),
        in_hbm(node_gain),
        in_hbm(node_shift),
    )
    return pl.pallas_call(
        hand_out,
        out_shape=(
            jax.ShapeDtypeStruct(edge_feats.shape, BF16),
            jax.ShapeDtypeStruct(node_feats.shape, BF16),
        ),
        in_specs=[vmem, vmem],
        out_specs=(hbm, hbm),
        scratch_shapes=[dma, dma],
        compiler_params=pltpu.CompilerParams(vmem_limit_bytes=2**20),
        name="hand_out",
    )(*(pltpu.with_memory_space_constraint(value, pltpu.VMEM) for value in finished))


def solution(mesh):
    return jax.shard_map(
        per_device,
        mesh=mesh,
        in_specs=(
            P(("graph", "feat"), None),
            P(("graph", "feat"), None),
            P(("graph", "feat")),
            P(("graph", "feat")),
            P("graph", None, None),
            P("graph"),
            P(),
            P(),
            P(),
            P(),
            P(),
            P(),
            P(),
            P(),
        ),
        out_specs=(P(("graph", "feat"), None), P(("graph", "feat"), None)),
        check_vma=False,
    )
```
